32 devices in a mesh: row: 16 (over z, x, core), feat: 2 (over y).
Axes of the slice: x: 2, y: 2, z: 4, core: 2. Of those that a mesh axis runs over, the one named last changes fastest.
Arguments:
- bin_index: int32 [1024, 49152], P('feat', 'row'), may hold values from 0 to 63
- gradient: bfloat16 [32, 49152], P(None, ('row', 'feat')), may hold values from -6 to 6
- hessian: bfloat16 [49152], P(('row', 'feat')), may hold values from 0.25 to 4
- row_node: int32 [49152], P('row'), may hold values from 0 to 7
Outputs:
- split_gain: float32 [1024, 512], P(('feat', 'row'))
- best_gain: float32 [8], replicated
The draws below stay inside these ranges and needn't reach their ends.
All inputs are finite; a program needn't handle non-finite values.
Results may differ from the reference program's by a relative error of at most 0.0003.
Values may be sent and summed in bfloat16 or wider, within the bound.
A program may use at most 128 MiB of HBM per device.

```python
import math
import jax
import jax.numpy as jnp
from jax import lax

FEATURES = 1024
OUTPUTS = 32
BINS = 64
NODES = 8
ROWS = 49152


def plant(values, stream_key, smallest, high):
    place = [jax.random.randint(jax.random.fold_in(stream_key, axis), (), 0, length) for axis, length in enumerate(values.shape)]
    longest = values.shape.index(max(values.shape))
    beside = place[:longest] + [(place[longest] + 1) % values.shape[longest]] + place[longest + 1:]
    return values.at[tuple(place)].set(smallest).at[tuple(beside)].set(high)


def steps_of(key, dims, split, smallest, high):
    loudness, own = 1.0, jax.random.fold_in(key, 6)
    for position, blocks in split:
        draws = jnp.exp(jax.random.uniform(jax.random.fold_in(own, position), (blocks,), jnp.float32, smallest / len(split), high / len(split)))
        loudness = loudness * jnp.repeat(draws, dims[position] // blocks).reshape([-1 if axis == position else 1 for axis in range(len(dims))])
    return loudness


def normal_values(stream_key, extent, deviation, limit, split=(), held_as=jnp.bfloat16):
    values = jax.random.normal(stream_key, extent, jnp.float32) * deviation
    if len(split) > 0:
        values = steps_of(stream_key, extent, split, -0.22, 0.18) * values
    return jnp.clip(values, min=-limit, max=limit).astype(held_as)


def setup_inputs(seed: int = 0) -> dict:
    key_list = jax.random.split(jax.random.key(seed), 5)
    bin_index = plant(jax.random.randint(key_list[0], (FEATURES, ROWS), 0, BINS), jax.random.fold_in(key_list[0], 1), 0, BINS - 1).astype(jnp.int32)
    gradient = normal_values(key_list[1], (OUTPUTS, ROWS), 1.0, 6.0, ((1, 32),))
    hessian = jnp.clip(jnp.exp(math.log(4.0) - 2.7725887 * jax.random.uniform(key_list[2], (ROWS,), jnp.float32) ** steps_of(key_list[2], (ROWS,), ((0, 32),), -0.2, 0.2)), 0.25, 4.0).astype(jnp.bfloat16)
    row_node = plant(jax.random.randint(key_list[3], (ROWS,), 0, NODES), jax.random.fold_in(key_list[3], 1), 0, NODES - 1).astype(jnp.int32)
    return {"bin_index": bin_index, "gradient": gradient, "hessian": hessian, "row_node": row_node}


ridge_term = 1.0


def score_splits(histogram, whole_sums):
    left_sums = jnp.cumsum(histogram, axis=1)
    right_sums = whole_sums - left_sums

    def part_score(sums):
        return jnp.sum(sums[..., :-1] * sums[..., :-1], axis=-1) / (sums[..., -1] + ridge_term)

    outputs_count = histogram.shape[-1] - 1
    score_terms = part_score(left_sums) + part_score(right_sums) - part_score(whole_sums)
    return jnp.transpose((0.5 / outputs_count) * score_terms, (0, 2, 1))


def reference(bin_index, gradient, hessian, row_node):
    stacked = jnp.concatenate([gradient, hessian[None, :]], 0)
    stacked_rows = stacked.astype(jnp.float32).T
    node_ids = row_node.astype(jnp.int32)
    node_totals = jax.ops.segment_sum(stacked_rows, node_ids, num_segments=NODES)

    def one_feature(feature_bins):
        cell_ids = (node_ids * BINS + feature_bins.astype(jnp.int32)).astype(jnp.int32)
        sums = jax.ops.segment_sum(stacked_rows, cell_ids, num_segments=NODES * BINS)
        return jnp.transpose(sums.reshape(NODES, BINS, -1), (1, 0, 2))

    histogram = lax.map(one_feature, bin_index)
    split_gain = score_splits(histogram, node_totals[None, None])
    best_gain = jnp.max(split_gain, axis=(0, 2))
    return split_gain.reshape(FEATURES, NODES * BINS), best_gain
```

```python
import functools
import math

import jax
import jax.numpy as jnp
from jax import lax
from jax.experimental import pallas as pl
from jax.experimental.pallas import tpu as pltpu
from jax.sharding import PartitionSpec as P

BINS = 64
NODES = 8
GROUP = 4
CHUNKS = 4

ridge_term = 1.0


def gain_kernel(outputs_count, bins_ref, rows_ref, gain_ref, masked_ref, sums_ref):
    step = pl.program_id(0)
    features = bins_ref.shape[1]
    subs, width = rows_ref.shape[1], rows_ref.shape[3]
    group = math.gcd(features, GROUP)
    columns = group * BINS
    channels = outputs_count + 1

    for sub in range(subs):
        block = rows_ref[0, sub].astype(jnp.float32)
        nodes = block[channels : channels + 1]
        levels = lax.broadcasted_iota(jnp.int32, (NODES, 1), 0).astype(jnp.float32)
        picked = nodes == levels
        masked = jnp.concatenate(
            [jnp.where(picked, block[k : k + 1], 0.0) for k in range(channels)], 0
        )
        masked_ref[:, sub * width : (sub + 1) * width] = masked.astype(jnp.bfloat16)

    masked = masked_ref[...]
    levels = lax.broadcasted_iota(jnp.int32, (BINS, 1), 0).astype(jnp.bfloat16)
    one, zero = jnp.bfloat16(1), jnp.bfloat16(0)
    for g in range(features // group):
        below = jnp.concatenate(
            [
                jnp.where(bins_ref[0, g * group + j : g * group + j + 1, :] <= levels, one, zero)
                for j in range(group)
            ],
            0,
        )
        part = lax.dot_general(
            masked, below, (((1,), (1,)), ((), ())), preferred_element_type=jnp.float32
        )
        where = slice(g * columns, (g + 1) * columns)

        @pl.when(step == 0)
        def _():
            sums_ref[:, where] = part

        @pl.when(step > 0)
        def _():
            sums_ref[:, where] += part

    @pl.when(step == pl.num_programs(0) - 1)
    def _():
        for g in range(features // group):
            where = slice(g * columns, (g + 1) * columns)
            left2 = right2 = whole2 = 0.0
            for k in range(channels):
                left = sums_ref[k * NODES : (k + 1) * NODES, where]
                whole = sums_ref[k * NODES : (k + 1) * NODES, BINS - 1 : BINS]
                right = whole - left
                if k < outputs_count:
                    left2 = left2 + left * left
                    right2 = right2 + right * right
                    whole2 = whole2 + whole * whole
            gain_ref[:, where] = (0.5 / outputs_count) * (
                left2 / (left + ridge_term)
                + right2 / (right + ridge_term)
                - whole2 / (whole + ridge_term)
            )


def chunk_gain(bins, rows, outputs_count):
    shards, features, shard_rows = bins.shape
    subs, width = rows.shape[1], rows.shape[3]
    sums_rows = (outputs_count + 1) * NODES
    flops = 2 * sums_rows * features * BINS * shards * shard_rows
    return pl.pallas_call(
        functools.partial(gain_kernel, outputs_count),
        out_shape=jax.ShapeDtypeStruct((NODES, features * BINS), jnp.float32),
        grid=(shards,),
        in_specs=[
            pl.BlockSpec((1, features, shard_rows), lambda i: (i, 0, 0)),
            pl.BlockSpec((1, subs, rows.shape[2], width), lambda i: (i, 0, 0, 0)),
        ],
        out_specs=pl.BlockSpec((NODES, features * BINS), lambda i: (0, 0)),
        scratch_shapes=[
            pltpu.VMEM((sums_rows, shard_rows), jnp.bfloat16),
            pltpu.VMEM((sums_rows, features * BINS), jnp.float32),
        ],
        compiler_params=pltpu.CompilerParams(
            dimension_semantics=("arbitrary",), vmem_limit_bytes=32 * 1024 * 1024
        ),
        cost_estimate=pl.CostEstimate(
            flops=flops, bytes_accessed=2 * (bins.size + rows.size), transcendentals=0
        ),
        name="chunk_gain",
    )(bins, rows)


def on_device(bin_index, gradient, hessian, row_node):
    shards, subs = lax.axis_size("row"), lax.axis_size("feat")
    owned = bin_index.shape[0] // shards
    outputs_count, width = gradient.shape
    shard_rows = bin_index.shape[1]
    nodes = lax.dynamic_slice_in_dim(row_node, lax.axis_index("feat") * width, width, 0)
    mine = jnp.concatenate(
        [gradient, hessian[None], nodes[None].astype(jnp.bfloat16)], 0
    )
    rows = lax.all_gather(mine, ("row", "feat"), axis=0, tiled=False)
    rows = rows.reshape(shards, subs, outputs_count + 2, width)

    chunks = math.gcd(CHUNKS, max(owned // GROUP, 1))
    span = owned // chunks
    bins = bin_index.reshape(shards, owned, shard_rows)
    gains = []
    for c in range(chunks):
        part = bins[:, c * span : (c + 1) * span].astype(jnp.bfloat16)
        part = lax.all_to_all(part, "row", 0, 0)
        gains.append(chunk_gain(part, rows, outputs_count))
    gain = jnp.concatenate(gains, 1)
    best_gain = lax.pmax(jnp.max(gain, axis=1), ("row", "feat"))
    split_gain = gain.reshape(NODES, owned, BINS).transpose(1, 0, 2)
    return (split_gain.reshape(owned, NODES * BINS), best_gain)


def solution(mesh):
    in_specs = (P("feat", "row"), P(None, ("row", "feat")), P(("row", "feat")), P("row"))
    out_specs = (P(("feat", "row"), None), P())
    return jax.shard_map(
        on_device, mesh=mesh, in_specs=in_specs, out_specs=out_specs, check_vma=False
    )
```

```python
import functools
import math

import jax
import jax.numpy as jnp
from jax import lax
from jax.experimental import pallas as pl
from jax.experimental.pallas import tpu as pltpu
from jax.sharding import PartitionSpec as P

BINS = 64
NODES = 8
GROUP = 4
CHUNKS = 2

ridge_term = 1.0


def gain_kernel(outputs_count, bins_ref, rows_ref, gain_ref, masked_ref, sums_ref):
    step = pl.program_id(0)
    features = bins_ref.shape[1]
    subs, width = rows_ref.shape[1], rows_ref.shape[3]
    group = math.gcd(features, GROUP)
    columns = group * BINS
    channels = outputs_count + 1

    for sub in range(subs):
        block = rows_ref[0, sub].astype(jnp.float32)
        nodes = block[channels : channels + 1]
        levels = lax.broadcasted_iota(jnp.int32, (NODES, 1), 0).astype(jnp.float32)
        picked = nodes == levels
        masked = jnp.concatenate(
            [jnp.where(picked, block[k : k + 1], 0.0) for k in range(channels)], 0
        )
        masked_ref[:, sub * width : (sub + 1) * width] = masked.astype(jnp.bfloat16)

    masked = masked_ref[...]
    levels = lax.broadcasted_iota(jnp.int32, (BINS, 1), 0).astype(jnp.bfloat16)
    one, zero = jnp.bfloat16(1), jnp.bfloat16(0)
    for g in range(features // group):
        below = jnp.concatenate(
            [
                jnp.where(bins_ref[0, g * group + j : g * group + j + 1, :] <= levels, one, zero)
                for j in range(group)
            ],
            0,
        )
        part = lax.dot_general(
            masked, below, (((1,), (1,)), ((), ())), preferred_element_type=jnp.float32
        )
        where = slice(g * columns, (g + 1) * columns)

        @pl.when(step == 0)
        def _():
            sums_ref[:, where] = part

        @pl.when(step > 0)
        def _():
            sums_ref[:, where] += part

    @pl.when(step == pl.num_programs(0) - 1)
    def _():
        for g in range(features // group):
            where = slice(g * columns, (g + 1) * columns)
            left2 = right2 = whole2 = 0.0
            for k in range(channels):
                left = sums_ref[k * NODES : (k + 1) * NODES, where]
                whole = sums_ref[k * NODES : (k + 1) * NODES, BINS - 1 : BINS]
                right = whole - left
                if k < outputs_count:
                    left2 = left2 + left * left
                    right2 = right2 + right * right
                    whole2 = whole2 + whole * whole
            gain_ref[:, where] = (0.5 / outputs_count) * (
                left2 / (left + ridge_term)
                + right2 / (right + ridge_term)
                - whole2 / (whole + ridge_term)
            )


def chunk_gain(bins, rows, outputs_count):
    shards, features, shard_rows = bins.shape
    subs, width = rows.shape[1], rows.shape[3]
    sums_rows = (outputs_count + 1) * NODES
    flops = 2 * sums_rows * features * BINS * shards * shard_rows
    return pl.pallas_call(
        functools.partial(gain_kernel, outputs_count),
        out_shape=jax.ShapeDtypeStruct((NODES, features * BINS), jnp.float32),
        grid=(shards,),
        in_specs=[
            pl.BlockSpec((1, features, shard_rows), lambda i: (i, 0, 0)),
            pl.BlockSpec((1, subs, rows.shape[2], width), lambda i: (i, 0, 0, 0)),
        ],
        out_specs=pl.BlockSpec((NODES, features * BINS), lambda i: (0, 0)),
        scratch_shapes=[
            pltpu.VMEM((sums_rows, shard_rows), jnp.bfloat16),
            pltpu.VMEM((sums_rows, features * BINS), jnp.float32),
        ],
        compiler_params=pltpu.CompilerParams(
            dimension_semantics=("arbitrary",), vmem_limit_bytes=32 * 1024 * 1024
        ),
        cost_estimate=pl.CostEstimate(
            flops=flops, bytes_accessed=2 * (bins.size + rows.size), transcendentals=0
        ),
        name="chunk_gain",
    )(bins, rows)


def on_device(bin_index, gradient, hessian, row_node):
    shards, subs = lax.axis_size("row"), lax.axis_size("feat")
    owned = bin_index.shape[0] // shards
    outputs_count, width = gradient.shape
    shard_rows = bin_index.shape[1]
    nodes = lax.dynamic_slice_in_dim(row_node, lax.axis_index("feat") * width, width, 0)
    mine = jnp.concatenate(
        [gradient, hessian[None], nodes[None].astype(jnp.bfloat16)], 0
    )
    rows = lax.all_gather(mine, ("row", "feat"), axis=0, tiled=False)
    rows = rows.reshape(shards, subs, outputs_count + 2, width)

    chunks = math.gcd(CHUNKS, max(owned // GROUP, 1))
    span = owned // chunks
    bins = bin_index.reshape(shards, owned, shard_rows)
    gains = []
    for c in range(chunks):
        part = bins[:, c * span : (c + 1) * span].astype(jnp.bfloat16)
        part = lax.all_to_all(part, "row", 0, 0)
        gains.append(chunk_gain(part, rows, outputs_count))
    gain = jnp.concatenate(gains, 1)
    best_gain = lax.pmax(jnp.max(gain, axis=1), ("row", "feat"))
    split_gain = gain.reshape(NODES, owned, BINS).transpose(1, 0, 2)
    return (split_gain.reshape(owned, NODES * BINS), best_gain)


def solution(mesh):
    in_specs = (P("feat", "row"), P(None, ("row", "feat")), P(("row", "feat")), P("row"))
    out_specs = (P(("feat", "row"), None), P())
    return jax.shard_map(
        on_device, mesh=mesh, in_specs=in_specs, out_specs=out_specs, check_vma=False
    )
```
